16 devices in a mesh: tp: 2 (over z), cp: 8 (over y, x, core).
Axes of the slice: x: 2, y: 2, z: 2, core: 2. Of those that a mesh axis runs over, the one named last changes fastest.
Arguments:
- x_in: bfloat16 [32, 2048, 1024], P(None, 'cp')
- grad_z: bfloat16 [32, 2048, 1024], P(None, 'cp')
- seg_pos: int32 [32, 2048], P(None, 'cp')
- norm_scale: bfloat16 [1024], replicated
- w_x: bfloat16 [1024, 1024], P(None, 'tp')
- b_x: bfloat16 [1024], P('tp')
- w_y: bfloat16 [1024, 1024], P(None, 'tp')
- b_y: bfloat16 [1024], P('tp')
- conv_w: bfloat16 [4, 1024], P(None, 'tp')
- conv_b: bfloat16 [1024], P('tp')
- w_a: bfloat16 [8, 128, 128], P('tp')
- b_a: bfloat16 [1024], P('tp')
- w_i: bfloat16 [8, 128, 128], P('tp')
- b_i: bfloat16 [1024], P('tp')
- a_param: float32 [1024], P('tp')
- w_out: bfloat16 [1024, 1024], P('tp')
- b_out: bfloat16 [1024], replicated
Outputs:
- output 1: bfloat16 [32, 2048, 1024], P(None, 'cp')
- output 2: bfloat16 [32, 2048, 1024], P(None, 'cp')
- output 3: float32 [1024], replicated
- output 4: float32 [1024, 1024], P(None, 'tp')
- output 5: float32 [1024], P('tp')
- output 6: float32 [1024, 1024], P(None, 'tp')
- output 7: float32 [1024], P('tp')
- output 8: float32 [4, 1024], P(None, 'tp')
- output 9: float32 [1024], P('tp')
- output 10: float32 [8, 128, 128], P('tp')
- output 11: float32 [1024], P('tp')
- output 12: float32 [8, 128, 128], P('tp')
- output 13: float32 [1024], P('tp')
- output 14: float32 [1024], P('tp')
- output 15: float32 [1024, 1024], P('tp')
- output 16: float32 [1024], replicated
All inputs are finite; a program needn't handle non-finite values.
Results may differ from the reference program's by a relative error of at most 0.00761529.
Values sent between devices are 32-bit elements.
A program may use at most 1 GiB of HBM per device.

```python
import math
import jax
import jax.numpy as jnp
from jax import lax

BATCH_SEQS = 32
SEQ_LEN = 2048
D_MODEL = 1024
D_RNN = 1024
GATE_BLOCKS = 8
DOC_STARTS = 2
CONV_WIDTH = 4
BLOCK_WIDTH = D_RNN // GATE_BLOCKS
NORM_EPS = 1e-6


def doc_positions(pos_key):
    starts = jax.random.randint(pos_key, (BATCH_SEQS, DOC_STARTS), 1, SEQ_LEN)
    step_ids = jnp.arange(SEQ_LEN, dtype=jnp.int32)
    is_start = jnp.any(step_ids[None, :, None] == starts[:, None, :], axis=-1) | (step_ids == 0)[None, :]
    last_start = lax.cummax(jnp.where(is_start, step_ids[None, :], 0), axis=1)
    return (step_ids[None, :] - last_start).astype(jnp.int32)


def setup_inputs(seed: int = 0) -> dict:
    key_list = jax.random.split(jax.random.key(seed), 17)

    def draw_normal(key_index, arr_shape, factor):
        return jax.random.normal(key_list[key_index], arr_shape, jnp.float32) * factor

    tok_shape = (BATCH_SEQS, SEQ_LEN, D_MODEL)
    gate_shape = (GATE_BLOCKS, BLOCK_WIDTH, BLOCK_WIDTH)
    soft_plus = jnp.exp(jax.random.uniform(key_list[14], (D_RNN,), jnp.float32, math.log(2e-5), math.log(2e-4)))
    return {
        "x_in": draw_normal(0, tok_shape, 1.0).astype(jnp.bfloat16),
        "grad_z": draw_normal(1, tok_shape, 1.0).astype(jnp.bfloat16),
        "seg_pos": doc_positions(key_list[2]),
        "norm_scale": draw_normal(3, (D_MODEL,), 0.3).astype(jnp.bfloat16),
        "w_x": draw_normal(4, (D_MODEL, D_RNN), D_MODEL ** -0.5).astype(jnp.bfloat16),
        "b_x": draw_normal(5, (D_RNN,), 0.3).astype(jnp.bfloat16),
        "w_y": draw_normal(6, (D_MODEL, D_RNN), D_MODEL ** -0.5).astype(jnp.bfloat16),
        "b_y": draw_normal(7, (D_RNN,), 0.3).astype(jnp.bfloat16),
        "conv_w": draw_normal(8, (CONV_WIDTH, D_RNN), 0.5).astype(jnp.bfloat16),
        "conv_b": draw_normal(9, (D_RNN,), 0.3).astype(jnp.bfloat16),
        "w_a": draw_normal(10, gate_shape, BLOCK_WIDTH ** -0.5).astype(jnp.bfloat16),
        "b_a": draw_normal(11, (D_RNN,), 0.5).astype(jnp.bfloat16),
        "w_i": draw_normal(12, gate_shape, BLOCK_WIDTH ** -0.5).astype(jnp.bfloat16),
        "b_i": draw_normal(13, (D_RNN,), 0.5).astype(jnp.bfloat16),
        "a_param": jnp.log(jnp.expm1(soft_plus)),
        "w_out": draw_normal(15, (D_RNN, D_MODEL), D_RNN ** -0.5).astype(jnp.bfloat16),
        "b_out": draw_normal(16, (D_MODEL,), 0.3).astype(jnp.bfloat16),
    }


def to_bf16(arr_val):
    return arr_val + lax.stop_gradient(arr_val.astype(jnp.bfloat16).astype(jnp.float32) - arr_val)


def block_forward(x_f, norm_scale, w_x, b_x, w_y, b_y, conv_w, conv_b, w_a, b_a, w_i, b_i, a_param, w_out, b_out, seg_pos):
    mean_sq = jnp.mean(x_f * x_f, axis=-1, keepdims=True)
    normed = to_bf16(x_f * lax.rsqrt(mean_sq + NORM_EPS) * (1.0 + norm_scale))
    y_act = jax.nn.gelu(jnp.dot(normed, w_y, preferred_element_type=jnp.float32) + b_y, approximate=True)
    x_branch = to_bf16(jnp.dot(normed, w_x, preferred_element_type=jnp.float32) + b_x)
    batch_n, seq_n, width_n = x_branch.shape
    conv_sum = x_branch * conv_w[0] + conv_b
    for tap_k in range(1, CONV_WIDTH):
        shifted = jnp.pad(x_branch[:, :seq_n - tap_k], ((0, 0), (tap_k, 0), (0, 0)))
        keep_mask = (seg_pos >= tap_k)[:, :, None]
        conv_sum = conv_sum + jnp.where(keep_mask, shifted, 0.0) * conv_w[tap_k]
    conv_out = to_bf16(conv_sum)
    blocks = conv_out.reshape(batch_n, seq_n, GATE_BLOCKS, BLOCK_WIDTH)
    pre_a = jnp.einsum("bthk,hkj->bthj", blocks, w_a).reshape(batch_n, seq_n, width_n) + b_a
    pre_i = jnp.einsum("bthk,hkj->bthj", blocks, w_i).reshape(batch_n, seq_n, width_n) + b_i
    reset_mask = (seg_pos == 0)[:, :, None]
    log_a = -8.0 * jax.nn.sigmoid(pre_a) * jax.nn.softplus(a_param)
    decays = jnp.where(reset_mask, 0.0, jnp.exp(log_a))
    multiplier = jnp.where(reset_mask, 1.0, jnp.sqrt(-jnp.expm1(2.0 * log_a)))
    drives = multiplier * jax.nn.sigmoid(pre_i) * conv_out

    def scan_step(carry_h, inputs_t):
        next_h = inputs_t[0] * carry_h + inputs_t[1]
        return next_h, next_h

    init_h = jnp.zeros((batch_n, width_n), jnp.float32)
    _, hidden_t = lax.scan(scan_step, init_h, (jnp.swapaxes(decays, 0, 1), jnp.swapaxes(drives, 0, 1)))
    hidden = jnp.swapaxes(hidden_t, 0, 1)
    mixed_v = to_bf16(hidden * y_act)
    out_proj = jnp.dot(mixed_v, w_out, preferred_element_type=jnp.float32) + b_out
    return to_bf16(x_f + out_proj)


def reference(x_in, grad_z, seg_pos, norm_scale, w_x, b_x, w_y, b_y, conv_w, conv_b, w_a, b_a, w_i, b_i, a_param, w_out, b_out):
    primals = [param_arr.astype(jnp.float32) for param_arr in (x_in, norm_scale, w_x, b_x, w_y, b_y, conv_w, conv_b, w_a, b_a, w_i, b_i, a_param, w_out, b_out)]

    def run_block(*params):
        return block_forward(*params, seg_pos)

    z_val, pull_back = jax.vjp(run_block, *primals)
    grad_list = pull_back(grad_z.astype(jnp.float32))
    return (z_val.astype(jnp.bfloat16), grad_list[0].astype(jnp.bfloat16), grad_list[1], grad_list[2], grad_list[3], grad_list[4], grad_list[5], grad_list[6], grad_list[7], grad_list[8], grad_list[9], grad_list[10], grad_list[11], grad_list[12], grad_list[13], grad_list[14])
```

```python
import functools
import jax
import jax.numpy as jnp
import numpy as np
from jax import lax
from jax.experimental import pallas as pl
from jax.experimental.pallas import tpu as pltpu
from jax.sharding import PartitionSpec as P

NORM_EPS = 1e-6
CONV_WIDTH = 4
BORROW = CONV_WIDTH - 1
LANES = 128
TB = 16
TINY = 1e-37
VMEM_BYTES = 66 * 1000 * 1000
F32 = jnp.float32
BF16 = jnp.bfloat16
IN_SPECS = (P(None, "cp", None), P(None, "cp", None), P(None, "cp"), P(), P(None, "tp"), P("tp"), P(None, "tp"), P("tp"), P(None, "tp"), P("tp"), P("tp", None, None), P("tp"), P("tp", None, None), P("tp"), P("tp"), P("tp", None), P())
OUT_SPECS = (P(None, "cp", None), P(None, "cp", None), P(), P(None, "tp"), P("tp"), P(None, "tp"), P("tp"), P(None, "tp"), P("tp"), P("tp", None, None), P("tp"), P("tp", None, None), P("tp"), P("tp"), P("tp", None), P())
V_BX, V_BY, V_CW, V_CB, V_BA, V_BI, V_SP = 0, 1, 2, 6, 7, 8, 9
S_BX, S_BY, S_CW, S_CB, S_BA, S_BI, S_AP = 0, 1, 2, 6, 7, 8, 9
LOG2E = 1.4426950408889634
RESET_LOG = -1e4
GELU_C = 0.7978845608028654
GELU_D = 0.044715


def dot_nn(lhs, rhs):
    return lax.dot_general(lhs, rhs, (((1,), (0,)), ((), ())), preferred_element_type=F32)


def dot_nt(lhs, rhs):
    return lax.dot_general(lhs, rhs, (((1,), (1,)), ((), ())), preferred_element_type=F32)


def dot_tn(lhs, rhs):
    return lax.dot_general(lhs, rhs, (((0,), (0,)), ((), ())), preferred_element_type=F32)


def sigm_scaled(val, bias):
    root = lax.rsqrt(1.0 + jnp.exp2(val * (-LOG2E) + bias))
    return root * root


def fold8(val):
    return (val[0:8] + val[8:16]) + (val[16:24] + val[24:32])


def to_time_major(perm, src_ref, dst_ref):
    n_seq, _, width = src_ref.shape
    for h in range(n_seq // TB):
        rows = src_ref[h * TB:(h + 1) * TB].reshape(TB * TB, width)
        dst_ref[:, h * TB:(h + 1) * TB, :] = dot_nn(perm, rows).astype(BF16).reshape(TB, TB, width)


def to_batch_major(perm, src_ref, dst_ref):
    n_seq, width = src_ref.shape[1], src_ref.shape[2]
    for h in range(n_seq // TB):
        rows = src_ref[:, h * TB:(h + 1) * TB, :].reshape(TB * TB, width)
        dst_ref[h * TB:(h + 1) * TB] = dot_nn(perm, rows).astype(BF16).reshape(TB, TB, width)


def norm_rows(xf, gain):
    rs = lax.rsqrt(jnp.mean(xf * xf, axis=-1, keepdims=True) + NORM_EPS)
    return (xf * rs * gain).astype(BF16)


def chunk_vec(vec_ref, col):
    return lambda row: vec_ref[row:row + 1, col]


def gate_terms(pa, pi, vec, cap):
    r = sigm_scaled(pa, vec(V_BA))
    i = sigm_scaled(pi, vec(V_BI))
    log_a = jnp.minimum(vec(V_SP) * r, cap)
    a = jnp.exp(log_a)
    a2 = a * a
    m2 = jnp.tanh(log_a) * (-1.0 - a2)
    inv_m = lax.rsqrt(jnp.maximum(m2, TINY))
    return r, i, log_a, a, a2, m2 * inv_m, inv_m


def gelu_parts(p):
    p2 = p * p
    half = 0.5 * jnp.tanh(p * (GELU_C + (GELU_C * GELU_D) * p2)) + 0.5
    y = p * half
    slope = half + y * (1.0 - half) * (2.0 * GELU_C + (6.0 * GELU_C * GELU_D) * p2)
    return y, slope


def gelu_only(p):
    return p * (0.5 * jnp.tanh(p * (GELU_C + (GELU_C * GELU_D) * (p * p))) + 0.5)


def fill_masks(pos_ref, mask_s):
    pos = pos_ref[...]
    mask_s[0] = jnp.where(pos == 0.0, RESET_LOG, 0.0)
    for k in range(1, CONV_WIDTH):
        mask_s[k] = jnp.where(pos >= float(k), 1.0, 0.0)


def lane_slice(start):
    return pl.ds(pl.multiple_of(start, LANES), LANES)


def row_slice(t, n_seq):
    return pl.ds(pl.multiple_of(t * n_seq, n_seq), n_seq)


def rows_at(t, n_seq):
    return slice(t * n_seq, (t + 1) * n_seq) if isinstance(t, int) else row_slice(t, n_seq)


def conv_lanes(mask_s, vec_ref, xb_ref, c_ref, n_seq, chunks):
    def conv_lane(l, c0):
        col = lane_slice(l * LANES)
        vec = chunk_vec(vec_ref, col)
        old = [xb_ref[l, rows_at(BORROW - k, n_seq), :].astype(F32) for k in range(1, CONV_WIDTH)]
        for t in range(TB):
            r = rows_at(t, n_seq)
            x = xb_ref[l, rows_at(t + BORROW, n_seq), :].astype(F32)
            acc = vec(V_CB) + x * vec(V_CW)
            for k in range(1, CONV_WIDTH):
                acc = acc + (old[k - 1] * mask_s[k, r, :]) * vec(V_CW + k)
            c_ref[l, r, :] = acc.astype(BF16)
            old = [x] + old[:-1]
        return c0

    lax.fori_loop(0, chunks, conv_lane, 0)


def gate_products(wai_ref, c_ref, pa_ref, pi_ref):
    for blk in range(wai_ref.shape[0]):
        pre = dot_nn(c_ref[blk], wai_ref[blk])
        pa_ref[blk] = pre[:, 0:LANES]
        pi_ref[blk] = pre[:, LANES:]


def put_chunks(ref, val, row0):
    for blk in range(ref.shape[0]):
        ref[blk, row0:row0 + val.shape[0], :] = val[:, blk * LANES:(blk + 1) * LANES].astype(ref.dtype)


def local_kernel(x_ref, gz_ref, pos_ref, xh_ref, vec_ref, sc_ref, wx_ref, wy_ref, wo_ref, wai_ref, perm_ref,
                 s_ref, r_ref, info_ref, xt_ref, gt_ref, n_ref, xb_ref, c_ref, py_ref, dm_ref, pa_ref, pi_ref,
                 nt_s, xbt_s, st_s, mask_s):
    n_seq, _, width = x_ref.shape
    own = wx_ref.shape[1]
    chunks = own // LANES
    rows = TB * n_seq
    halo = BORROW * n_seq
    perm = perm_ref[...]

    @pl.when(pl.program_id(0) == 0)
    def _():
        st_s[0] = jnp.zeros(st_s.shape[1:], F32)
        st_s[1] = jnp.ones(st_s.shape[1:], F32)
        st_s[2] = jnp.zeros(st_s.shape[1:], F32)
        for k in range(BORROW):
            nt_s[k * n_seq:(k + 1) * n_seq, :] = norm_rows(xh_ref[k * n_seq:(k + 1) * n_seq, :], sc_ref[0:1, :])
        put_chunks(xbt_s, dot_nn(nt_s[...], wx_ref[...]) + vec_ref[V_BX:V_BX + 1, :], 0)

    to_time_major(perm, x_ref, xt_ref)
    to_time_major(perm, gz_ref, gt_ref)
    n_ref[0, 0:halo, :] = nt_s[...]
    xb_ref[0, :, 0:halo, :] = xbt_s[...]

    fill_masks(pos_ref, mask_s)
    part = 2

    def norm_part(q, c):
        for k in range(part):
            t = q * part + k
            n_ref[0, row_slice(t + BORROW, n_seq), :] = norm_rows(xt_ref[t].astype(F32), sc_ref[0:1, :])
        return c

    lax.fori_loop(0, TB // part, norm_part, 0)
    n_blk = n_ref[0, halo:, :]
    put_chunks(xb_ref.at[0], dot_nn(n_blk, wx_ref[...]) + vec_ref[V_BX:V_BX + 1, :], halo)
    put_chunks(py_ref, dot_nn(n_blk, wy_ref[...]), 0)
    put_chunks(dm_ref, dot_nt(gt_ref[...].reshape(rows, width), wo_ref[...]), 0)
    nt_s[...] = n_ref[0, rows:, :]
    xbt_s[...] = xb_ref[0, :, rows:, :]
    conv_lanes(mask_s, vec_ref, xb_ref.at[0], c_ref, n_seq, chunks)
    gate_products(wai_ref, c_ref, pa_ref, pi_ref)

    def scan_lane(l, c0):
        col = lane_slice(l * LANES)
        vec = chunk_vec(vec_ref, col)

        def scan_t(t, carry):
            h, p, hg = carry
            r = row_slice(t, n_seq)
            _, i, _, a, _, m, _ = gate_terms(pa_ref[l, r, :], pi_ref[l, r, :], vec, mask_s[0, r, :])
            h = a * h + m * i * c_ref[l, r, :].astype(F32)
            p = a * p
            y = gelu_only(py_ref[l, r, :] + vec(V_BY))
            hg = hg + p * (dm_ref[l, r, :] * y)
            return h, p, hg

        h, p, hg = lax.fori_loop(0, TB, scan_t, (st_s[0, :, col], st_s[1, :, col], st_s[2, :, col]), unroll=2)
        st_s[0, :, col] = h
        st_s[1, :, col] = p
        st_s[2, :, col] = hg
        return c0

    lax.fori_loop(0, chunks, scan_lane, 0)
    s_ref[0] = st_s[0]
    r_ref[0] = st_s[1]
    info_ref[...] = st_s[...]


def far_kernel(n_ref, gt_ref, pos_ref, vec_ref, wxy_ref, wo_ref, wai_ref, c_ref, py_ref, dm_ref, pa_ref, pi_ref, xb_s, mask_s):
    n_seq, width = gt_ref.shape[1], gt_ref.shape[2]
    own = wo_ref.shape[0]
    rows = TB * n_seq
    halo = BORROW * n_seq

    @pl.when(pl.program_id(0) == 0)
    def _():
        put_chunks(xb_s, dot_nn(n_ref[0, 0:halo, :], wxy_ref[:, 0:own]) + vec_ref[V_BX:V_BX + 1, :], rows)

    xb_s[:, 0:halo, :] = xb_s[:, rows:, :]
    fill_masks(pos_ref, mask_s)
    n_blk = n_ref[0, halo:, :]
    put_chunks(xb_s, dot_nn(n_blk, wxy_ref[:, 0:own]) + vec_ref[V_BX:V_BX + 1, :], halo)
    put_chunks(py_ref, dot_nn(n_blk, wxy_ref[:, own:]), 0)
    put_chunks(dm_ref, dot_nt(gt_ref[...].reshape(rows, width), wo_ref[...]), 0)
    conv_lanes(mask_s, vec_ref, xb_s, c_ref, n_seq, own // LANES)
    gate_products(wai_ref, c_ref, pa_ref, pi_ref)


def compose_kernel(info_ref, _, out_ref, *, cp_size):
    cp_index = lax.axis_index("cp")
    tp_index = lax.axis_index("tp")
    n_seq, own = info_ref.shape[2], info_ref.shape[3]
    for side in range(2):
        base = jnp.where(side == 0, tp_index, 1 - tp_index) * cp_size
        state = jnp.zeros((n_seq, own), F32)
        grad = jnp.zeros((n_seq, own), F32)
        for q in range(cp_size):
            state = jnp.where(q < cp_index, info_ref[base + q, 1] * state + info_ref[base + q, 0], state)
        for q in range(cp_size - 1, -1, -1):
            grad = jnp.where(q > cp_index, info_ref[base + q, 1] * grad + info_ref[base + q, 2], grad)
        out_ref[0, :, side * own:(side + 1) * own] = state
        out_ref[1, :, side * own:(side + 1) * own] = grad


def norm_back(xf, dn, gain):
    rs = lax.rsqrt(jnp.mean(xf * xf, axis=-1, keepdims=True) + NORM_EPS)
    xh = xf * rs
    dg = dn * xh
    dx = rs * (dn * gain - xh * jnp.mean(dg * gain, axis=-1, keepdims=True))
    return dx, fold8(dg)


def main_kernel(gt_ref, n_ref, xb_ref, pos_ref, c0_ref, c1_ref, py0_ref, py1_ref, dm0_ref, dm1_ref, pa0_ref, pa1_ref, pi0_ref, pi1_ref,
                s0_ref, r0_ref, s1_ref, r1_ref, st_ref, vec_ref, sc_ref, wxy_ref, wai_ref, xh_ref,
                mix_ref, d_ref, gwx_ref, gwy_ref, gwo_ref, gwa_ref, gwi_ref, dxh_ref, gsh_ref,
                dpai_s, g_s, a_s, ka_s, ki_s, k1_s, k3_s, e_s, dh_s, gvec_s, mask_s):
    n_seq, width = gt_ref.shape[1], gt_ref.shape[2]
    chunks = c0_ref.shape[0]
    own = chunks * LANES
    rows = TB * n_seq
    halo = BORROW * n_seq
    step = pl.program_id(0)
    last = step == pl.num_programs(0) - 1

    @pl.when(step == 0)
    def _():
        e_s[...] = jnp.zeros_like(e_s)
        dh_s[...] = st_ref[1]
        for ref in (gwx_ref, gwy_ref, gwo_ref, gwa_ref, gwi_ref, gvec_s):
            ref[...] = jnp.zeros_like(ref)

    fill_masks(pos_ref, mask_s)
    g_rows = gt_ref[...].reshape(rows, width)

    def fwd_lane(side):
        c_ref, py_ref, dm_ref, pa_ref, pi_ref, s_ref, r_ref = ((c0_ref, py0_ref, dm0_ref, pa0_ref, pi0_ref, s0_ref, r0_ref), (c1_ref, py1_ref, dm1_ref, pa1_ref, pi1_ref, s1_ref, r1_ref))[side]

        def run(l, c0):
            loc = lane_slice(l * LANES)
            col = lane_slice(l * LANES + side * own)
            cola = lane_slice(2 * (l * LANES + side * own))
            coli = lane_slice(2 * (l * LANES + side * own) + LANES)
            coly = lane_slice(l * LANES + (2 * side + 1) * own)
            vec = chunk_vec(vec_ref, col)
            state = st_ref[0, :, col]
            state = jnp.where(last, state, s_ref[0, :, loc] + r_ref[0, :, loc] * state)

            h, s_by = state, jnp.zeros((8, LANES), F32)
            for t in range(TB):
                r = rows_at(t, n_seq)
                rg, i, log_a, a, a2, m, inv_m = gate_terms(pa_ref[l, r, :], pi_ref[l, r, :], vec, mask_s[0, r, :])
                cf = c_ref[l, r, :].astype(F32)
                k1 = m * i
                u = k1 * cf
                ah = a * h
                k3r = (ah - (i * cf) * (a2 * inv_m)) * rg
                h = ah + u
                y, slope = gelu_parts(py_ref[l, r, :] + vec(V_BY))
                dm = dm_ref[l, r, :]
                mix_ref[r, col] = (h * y).astype(BF16)
                dpy = dm * h * slope
                d_ref[r, coly] = dpy.astype(BF16)
                g_s[l + side * chunks, r, :] = dm * y
                a_s[l + side * chunks, r, :] = a
                k1_s[l + side * chunks, r, :] = k1
                ka_s[l + side * chunks, r, :] = k3r * (vec(V_SP) - log_a)
                ki_s[l + side * chunks, r, :] = u * (1.0 - i)
                if side == 0:
                    k3_s[l + side * chunks, r, :] = k3r
                    s_by = s_by + fold8(dpy)
            if side == 0:
                gvec_s[S_BY, :, col] += s_by
            return c0

        return run

    lax.fori_loop(0, chunks, fwd_lane(0), 0)
    lax.fori_loop(0, chunks, fwd_lane(1), 0)
    gwo_ref[...] += dot_tn(mix_ref[:, 0:own], g_rows)

    def bwd_lane(side):
        def run(l, c0):
            col = lane_slice(l * LANES + side * own)
            cola = lane_slice(2 * (l * LANES + side * own))
            coli = lane_slice(2 * (l * LANES + side * own) + LANES)

            def body(tt, carry):
                nxt, s_a, s_i, s_p = carry
                r = row_slice(TB - 1 - tt, n_seq)
                dh = g_s[l + side * chunks, r, :] + nxt
                nxt = a_s[l + side * chunks, r, :] * dh
                dpa = dh * ka_s[l + side * chunks, r, :]
                dpi = dh * ki_s[l + side * chunks, r, :]
                g_s[l + side * chunks, r, :] = dh * k1_s[l + side * chunks, r, :]
                dpai_s[l + side * chunks, r, 0:LANES] = dpa.astype(BF16)
                dpai_s[l + side * chunks, r, LANES:] = dpi.astype(BF16)
                if side == 0:
                    s_a = s_a + fold8(dpa)
                    s_i = s_i + fold8(dpi)
                    s_p = s_p + fold8(dh * k3_s[l + side * chunks, r, :])
                return nxt, s_a, s_i, s_p

            zero = jnp.zeros((8, LANES), F32)
            nxt, s_a, s_i, s_p = lax.fori_loop(0, TB, body, (dh_s[:, col], zero, zero, zero), unroll=4)
            dh_s[:, col] = nxt
            if side == 0:
                gvec_s[S_BA, :, col] += s_a
                gvec_s[S_BI, :, col] += s_i
                gvec_s[S_AP, :, col] += s_p
            return c0

        return run

    lax.fori_loop(0, chunks, bwd_lane(0), 0)
    lax.fori_loop(0, chunks, bwd_lane(1), 0)

    for blk in range(2 * chunks):
        g_s[blk] += dot_nt(dpai_s[blk], wai_ref[blk])
        if blk < chunks:
            g_ai = dot_tn(c0_ref[blk], dpai_s[blk])
            gwa_ref[blk] += g_ai[:, 0:LANES]
            gwi_ref[blk] += g_ai[:, LANES:]

    def convb_lane(side):
        def run(l, c0):
            col = lane_slice(l * LANES + side * own)
            colx = lane_slice(l * LANES + 2 * side * own)
            vec = chunk_vec(vec_ref, col)

            e1, e2, e3 = e_s[2 * n_seq:3 * n_seq, col], e_s[n_seq:2 * n_seq, col], e_s[0:n_seq, col]
            s_b = s_x = jnp.zeros((8, LANES), F32)
            taps = [s_b] * CONV_WIDTH
            if side == 0:
                xs = [xb_ref[0, l, rows_at(TB - 1 + BORROW - k, n_seq), :].astype(F32) for k in range(BORROW)]
            dc_next = g_s[l + side * chunks, rows_at(TB - 1, n_seq), :]
            for t in range(TB - 1, -1, -1):
                r = rows_at(t, n_seq)
                dc, dc_next = dc_next, g_s[l + side * chunks, rows_at(max(t - 1, 0), n_seq), :]
                dm = [dc] + [dc * mask_s[k, r, :] for k in range(1, CONV_WIDTH)]
                dx = e1 + dc * vec(V_CW)
                e1 = e2 + dm[1] * vec(V_CW + 1)
                e2 = e3 + dm[2] * vec(V_CW + 2)
                e3 = dm[3] * vec(V_CW + 3)
                d_ref[r, colx] = dx.astype(BF16)
                if side == 0:
                    s_b = s_b + fold8(dc)
                    s_x = s_x + fold8(dx)
                    xs = xs + [xb_ref[0, l, rows_at(t, n_seq), :].astype(F32)]
                    taps = [acc + fold8(dm[k] * xs[k]) for k, acc in enumerate(taps)]
                    xs = xs[1:]
            s0, s1, s2, s3 = taps
            e_s[2 * n_seq:3 * n_seq, col] = e1
            e_s[n_seq:2 * n_seq, col] = e2
            e_s[0:n_seq, col] = e3
            if side == 0:
                for row, val in ((S_CB, s_b), (S_BX, s_x), (S_CW, s0), (S_CW + 1, s1), (S_CW + 2, s2), (S_CW + 3, s3)):
                    gvec_s[row, :, col] += val
            return c0

        return run

    lax.fori_loop(0, chunks, convb_lane(0), 0)
    lax.fori_loop(0, chunks, convb_lane(1), 0)
    n_blk = n_ref[0, halo:, :]
    gwx_ref[...] += dot_tn(n_blk, d_ref[:, 0:own])
    gwy_ref[...] += dot_tn(n_blk, d_ref[:, own:2 * own])

    @pl.when(last)
    def _():
        e16 = e_s[...].astype(BF16)
        gwx_ref[...] += dot_tn(n_ref[0, 0:halo, :], e16[:, 0:own])
        gvec_s[S_BX] += fold8(e_s[0:n_seq, 0:own]) + fold8(e_s[n_seq:2 * n_seq, 0:own]) + fold8(e_s[2 * n_seq:, 0:own])
        dn = dot_nt(e16[:, 0:own], wxy_ref[:, 0:own]) + dot_nt(e16[:, own:], wxy_ref[:, 2 * own:3 * own])
        s_g = jnp.zeros((8, width), F32)
        for k in range(BORROW):
            sl = slice(k * n_seq, (k + 1) * n_seq)
            dx, sg = norm_back(xh_ref[sl, :], dn[sl], sc_ref[0:1, :])
            s_g = s_g + sg
            dxh_ref[sl, :] = dx
        gsh_ref[...] = s_g
        sums = jnp.sum(gvec_s[...], axis=1)
        for q in range(chunks):
            gwa_ref[chunks, q * 16:q * 16 + sums.shape[0], :] = sums[:, q * LANES:(q + 1) * LANES]


def out_kernel(mix_ref, d_ref, xt_ref, gt_ref, fix_ref, gsh_ref, sc_ref, wxy_ref, wo_ref, perm_ref, z_ref, gx_ref, gsc_ref, o_s, q_s, zt_s, gxt_s):
    n_seq, width = xt_ref.shape[1], xt_ref.shape[2]
    rows = TB * n_seq
    halo = BORROW * n_seq
    perm = perm_ref[...]
    step = pl.program_id(0)

    @pl.when(step == 0)
    def _():
        gsc_ref[0] = gsh_ref[...]
        gsc_ref[1] = jnp.zeros((8, width), F32)

    q_s[...] = dot_nt(d_ref[...], wxy_ref[...])
    part = 4

    def gx_part(q, c):
        rp = pl.ds(pl.multiple_of(q * part * n_seq, part * n_seq), part * n_seq)
        o_s[rp, :] = dot_nn(mix_ref[rp, :], wo_ref[...])
        for k in range(part):
            t = q * part + k
            r = row_slice(t, n_seq)
            dx, sg = norm_back(xt_ref[t].astype(F32), q_s[r, :], sc_ref[0:1, :])
            gzf = gt_ref[t].astype(F32)
            gx = gzf + dx
            q_s[r, :] = gx
            gxt_s[t] = gx.astype(BF16)
            gsc_ref[0] += sg
            gsc_ref[1] += fold8(gzf)
        return c

    lax.fori_loop(0, TB // part, gx_part, 0)

    @pl.when(step == pl.num_programs(0) - 1)
    def _():
        tail = q_s[rows - halo:, :] + fix_ref[...]
        gxt_s[TB - BORROW:] = tail.astype(BF16).reshape(BORROW, n_seq, width)

    def z_rows(t, c):
        zt_s[t] = (xt_ref[t].astype(F32) + (o_s[row_slice(t, n_seq), :] + sc_ref[1:2, :])).astype(BF16)
        return c

    lax.fori_loop(0, TB, z_rows, 0, unroll=2)
    to_batch_major(perm, zt_s, z_ref)
    to_batch_major(perm, gxt_s, gx_ref)


def pack_kernel(wx_ref, wy_ref, wo_ref, wa_ref, wi_ref, bx_ref, by_ref, cw_ref, cb_ref, ba_ref, bi_ref, sp_ref, half_ref, vec_ref, wai_ref):
    width, own = wx_ref.shape
    n_blk = wa_ref.shape[0]
    wai_ref[:, :, 0:LANES] = wa_ref[...]
    wai_ref[:, :, LANES:] = wi_ref[...]
    vec_ref[V_BX:V_BX + 1, :] = bx_ref[...].astype(F32).reshape(1, own)
    vec_ref[V_BY:V_BY + 1, :] = by_ref[...].astype(F32).reshape(1, own)
    vec_ref[V_CW:V_CW + CONV_WIDTH, :] = cw_ref[...].astype(F32)
    vec_ref[V_CB:V_CB + 1, :] = cb_ref[...].astype(F32).reshape(1, own)
    vec_ref[V_BA:V_BA + 1, :] = ba_ref[...].astype(F32).reshape(1, own) * (-LOG2E)
    vec_ref[V_BI:V_BI + 1, :] = bi_ref[...].astype(F32).reshape(1, own) * (-LOG2E)
    vec_ref[V_SP:V_SP + 1, :] = sp_ref[...].reshape(1, own)
    vec_ref[V_SP + 1:, :] = jnp.zeros((15 - V_SP, own), F32)
    for side, w_ref in enumerate((wx_ref, wy_ref)):
        @pl.when(lax.rem(lax.axis_index("cp"), 2) == side)
        def _():
            half_ref[0:width, :] = w_ref[...].astype(F32)
            half_ref[width:width + own, :] = wo_ref[:, side * own:(side + 1) * own].astype(F32)
            for k in range(n_blk // 2):
                blk = side * (n_blk // 2) + k
                half_ref[width + own:width + own + LANES, 2 * k * LANES:(2 * k + 1) * LANES] = wa_ref[blk].astype(F32)
                half_ref[width + own:width + own + LANES, (2 * k + 1) * LANES:(2 * k + 2) * LANES] = wi_ref[blk].astype(F32)
            half_ref[width + own + LANES:, :] = vec_ref[side * 8:(side + 1) * 8, :]


def assemble_kernel(wx_ref, wy_ref, wo_ref, wai_ref, vec_ref, mine_ref, other_ref, wxy_out, wo_out, wai_out, vec_out):
    width, own = wx_ref.shape
    n_blk = wai_ref.shape[0]
    wxy_out[:, 0:own] = wx_ref[...]
    wxy_out[:, own:2 * own] = wy_ref[...]
    wo_out[0:own, :] = wo_ref[...]
    wai_out[0:n_blk] = wai_ref[...]
    vec_out[:, 0:own] = vec_ref[...]
    parity = lax.rem(lax.axis_index("cp"), 2)
    for side in range(2):
        for ref, want in ((mine_ref, side), (other_ref, 1 - side)):
            @pl.when(parity == want)
            def _():
                wxy_out[:, (2 + side) * own:(3 + side) * own] = ref[0:width, :].astype(BF16)
                wo_out[own:, side * own:(side + 1) * own] = ref[width:width + own, :].astype(BF16)
                for k in range(n_blk // 2):
                    wai_out[n_blk + side * (n_blk // 2) + k] = ref[width + own:width + own + LANES, 2 * k * LANES:(2 * k + 2) * LANES].astype(BF16)
                vec_out[side * 8:(side + 1) * 8, own:] = ref[width + own + LANES:, :]


def const_spec(shape):
    return pl.BlockSpec(shape, lambda j: (0,) * len(shape), pipeline_mode=pl.Buffered(1))


def shard_body(x_in, grad_z, seg_pos, norm_scale, w_x, b_x, w_y, b_y, conv_w, conv_b, w_a, b_a, w_i, b_i, a_param, w_out, b_out, cp_size):
    n_seq, n_tok, width = x_in.shape
    own = w_x.shape[1]
    full = 2 * own
    nb = n_tok // TB
    rows = TB * n_seq
    halo = BORROW * n_seq
    chunks = own // LANES
    fwd_perm = [(d, d + 1) for d in range(cp_size - 1)]
    back_perm = [(d + 1, d) for d in range(cp_size - 1)]
    swap = [(0, 1), (1, 0)]

    x_tail = x_in[:, n_tok - BORROW:, :].astype(F32).transpose(1, 0, 2).reshape(halo, width)
    x_halo = lax.ppermute(x_tail, "cp", fwd_perm)

    sp8 = -8.0 * jax.nn.softplus(a_param)
    half, vec_own, w_ai = pl.pallas_call(
        pack_kernel,
        out_shape=[jax.ShapeDtypeStruct((width + own + LANES + 8, own), F32), jax.ShapeDtypeStruct((16, own), F32), jax.ShapeDtypeStruct((chunks, LANES, 2 * LANES), BF16)],
        compiler_params=pltpu.CompilerParams(vmem_limit_bytes=VMEM_BYTES),
        name="pack",
    )(w_x, w_y, w_out, w_a, w_i, b_x, b_y, conv_w, conv_b, b_a, b_i, sp8)
    far_half = lax.ppermute(half, "tp", swap)
    far_other = lax.ppermute(far_half, "cp", [(d, d ^ 1) for d in range(cp_size)])

    pos = jnp.broadcast_to(seg_pos.T.astype(F32).reshape(n_tok * n_seq, 1), (n_tok * n_seq, LANES))
    scales = jnp.concatenate([1.0 + norm_scale.astype(F32)[None], b_out.astype(F32)[None], jnp.zeros((6, width), F32)], axis=0)
    line = np.arange(TB * TB)
    perm = jnp.asarray((line[:, None] // TB == line[None, :] % TB) & (line[:, None] % TB == line[None, :] // TB), BF16)

    def vmem(shape, dtype):
        return pltpu.VMEM(shape, dtype)

    def sds(shape, dtype):
        return jax.ShapeDtypeStruct(shape, dtype)

    params = pltpu.CompilerParams(vmem_limit_bytes=VMEM_BYTES, dimension_semantics=("arbitrary",))

    def cost(gflop):
        return pl.CostEstimate(flops=gflop * 10 ** 9, bytes_accessed=10 ** 8, transcendentals=0)

    def blocks(idx):
        batch = pl.BlockSpec((n_seq, TB, width), lambda j: (0, idx(j), 0))
        time = pl.BlockSpec((TB, n_seq, width), lambda j: (idx(j), 0, 0))
        row = lambda cols: pl.BlockSpec((rows, cols), lambda j: (idx(j), 0))
        per = lambda *dims: pl.BlockSpec((1,) + dims, lambda j: (idx(j), 0, 0))
        chk = pl.BlockSpec((chunks, rows, LANES), lambda j: (0, idx(j), 0))
        xbs = pl.BlockSpec((1, chunks, rows + halo, LANES), lambda j: (idx(j), 0, 0, 0))
        return batch, time, row, per, chk, xbs

    batch, time, row, per, chk, xbs = blocks(lambda j: j)
    tok = n_tok * n_seq
    ends, prods, info, xt, gt, n_all, xb, c_own, py_own, dm_own, pa_own, pi_own = pl.pallas_call(
        local_kernel,
        grid=(nb,),
        in_specs=[batch, batch, row(LANES), const_spec((halo, width)), const_spec((16, own)), const_spec((8, width)),
                  const_spec((width, own)), const_spec((width, own)), const_spec((own, width)), const_spec(w_ai.shape), const_spec(perm.shape)],
        out_specs=[per(n_seq, own), per(n_seq, own), const_spec((3, n_seq, own)), time, time, per(rows + halo, width), xbs,
                   chk, chk, chk, chk, chk],
        out_shape=[sds((nb, n_seq, own), F32), sds((nb, n_seq, own), F32), sds((3, n_seq, own), F32), sds((n_tok, n_seq, width), BF16), sds((n_tok, n_seq, width), BF16),
                   sds((nb, rows + halo, width), BF16), sds((nb, chunks, rows + halo, LANES), BF16), sds((chunks, tok, LANES), BF16)] + [sds((chunks, tok, LANES), F32)] * 4,
        scratch_shapes=[vmem((halo, width), BF16), vmem((chunks, halo, LANES), BF16), vmem((3, n_seq, own), F32), vmem((CONV_WIDTH, rows, LANES), F32)],
        compiler_params=params, cost_estimate=cost(100), name="local_pass",
    )(x_in, grad_z, pos, x_halo, vec_own, scales, w_x, w_y, w_out, w_ai, perm)

    infos = lax.all_gather(info, ("tp", "cp"))
    far_ends = lax.ppermute(ends, "tp", swap)
    far_prods = lax.ppermute(prods, "tp", swap)

    w_xy, w_o, w_g, vec = pl.pallas_call(
        assemble_kernel,
        out_shape=[sds((width, 4 * own), BF16), sds((full, width), BF16), sds((2 * chunks,) + w_ai.shape[1:], BF16), sds((16, full), F32)],
        compiler_params=pltpu.CompilerParams(vmem_limit_bytes=VMEM_BYTES),
        name="assemble",
    )(w_x, w_y, w_out, w_ai, vec_own, far_half, far_other)

    c_far, py_far, dm_far, pa_far, pi_far = pl.pallas_call(
        far_kernel,
        grid=(nb,),
        in_specs=[per(rows + halo, width), time, row(LANES), pl.BlockSpec((16, own), lambda j: (0, 1), pipeline_mode=pl.Buffered(1)),
                  pl.BlockSpec((width, full), lambda j: (0, 1), pipeline_mode=pl.Buffered(1)), pl.BlockSpec((own, width), lambda j: (1, 0), pipeline_mode=pl.Buffered(1)),
                  pl.BlockSpec(w_ai.shape, lambda j: (1, 0, 0), pipeline_mode=pl.Buffered(1))],
        out_specs=[chk] * 5,
        out_shape=[sds((chunks, tok, LANES), BF16)] + [sds((chunks, tok, LANES), F32)] * 4,
        scratch_shapes=[vmem((chunks, rows + halo, LANES), BF16), vmem((CONV_WIDTH, rows, LANES), F32)],
        compiler_params=params, cost_estimate=cost(50), name="far_pass",
    )(n_all, gt, pos, vec, w_xy, w_o, w_g)

    states = pl.pallas_call(
        functools.partial(compose_kernel, cp_size=cp_size),
        in_specs=[pl.BlockSpec(memory_space=pltpu.VMEM), pl.BlockSpec(memory_space=pl.ANY)],
        out_shape=sds((2, n_seq, full), F32),
        compiler_params=pltpu.CompilerParams(vmem_limit_bytes=VMEM_BYTES),
        name="compose",
    )(infos, c_far)

    batch, time, row, per, chk, xbs = blocks(lambda j: nb - 1 - j)
    bound = pl.BlockSpec((1, n_seq, own), lambda j: (jnp.maximum(nb - 2 - j, 0), 0, 0))
    mix, d_all, g_wx, g_wy, g_wo, g_wa, g_wi, dx_halo, g_sh = pl.pallas_call(
        main_kernel,
        grid=(nb,),
        in_specs=[time, per(rows + halo, width), xbs, row(LANES)] + [chk] * 10 + [
                  bound, bound, bound, bound, const_spec((2, n_seq, full)), const_spec((16, full)), const_spec((8, width)),
                  const_spec((width, 2 * full)), const_spec(w_g.shape), const_spec((halo, width))],
        out_specs=[row(full), row(2 * full), const_spec((width, own)), const_spec((width, own)), const_spec((own, width)),
                   const_spec((chunks + 1, LANES, LANES)), const_spec((chunks, LANES, LANES)), const_spec((halo, width)), const_spec((8, width))],
        out_shape=[sds((tok, full), BF16), sds((tok, 2 * full), BF16), sds((width, own), F32), sds((width, own), F32), sds((own, width), F32),
                   sds((chunks + 1, LANES, LANES), F32), sds((chunks, LANES, LANES), F32), sds((halo, width), F32), sds((8, width), F32)],
        scratch_shapes=[vmem((2 * chunks, rows, 2 * LANES), BF16)] + [vmem((2 * chunks, rows, LANES), F32)] * 5 + [vmem((chunks, rows, LANES), F32), vmem((halo, full), F32), vmem((n_seq, full), F32), vmem((10, 8, own), F32), vmem((CONV_WIDTH, rows, LANES), F32)],
        compiler_params=params, cost_estimate=cost(300), name="main_pass",
    )(gt, n_all, xb, pos, c_own, c_far, py_own, py_far, dm_own, dm_far, pa_own, pa_far, pi_own, pi_far, ends, prods, far_ends, far_prods, states, vec, scales, w_xy, w_g, x_halo)

    fix = lax.ppermute(dx_halo, "cp", back_perm)
    g_wx, g_wy, g_wo, g_wa, g_wi = lax.psum((g_wx, g_wy, g_wo, g_wa, g_wi), "cp")

    batch, time, row, per, chk, xbs = blocks(lambda j: j)
    z_out, grad_x, g_sc = pl.pallas_call(
        out_kernel,
        grid=(nb,),
        in_specs=[row(full), row(2 * full), time, time, const_spec((halo, width)), const_spec((8, width)), const_spec((8, width)),
                  const_spec((width, 2 * full)), const_spec((full, width)), const_spec(perm.shape)],
        out_specs=[batch, batch, const_spec((2, 8, width))],
        out_shape=[sds(x_in.shape, BF16), sds(x_in.shape, BF16), sds((2, 8, width), F32)],
        scratch_shapes=[vmem((rows, width), F32), vmem((rows, width), F32), vmem((TB, n_seq, width), BF16), vmem((TB, n_seq, width), BF16)],
        compiler_params=params, cost_estimate=cost(100), name="out_pass",
    )(mix, d_all, xt, gt, fix, g_sh, scales, w_xy, w_o, perm)

    g_sc = jnp.sum(g_sc, axis=1)
    hop = 1
    while hop < cp_size:
        g_sc = g_sc + lax.ppermute(g_sc, "cp", [(d, d ^ hop) for d in range(cp_size)])
        hop *= 2

    sums = jnp.concatenate([g_wa[chunks, q * 16:q * 16 + 10, :] for q in range(chunks)], axis=1)
    g_ap = sums[S_AP] * (-8.0) * jax.nn.sigmoid(a_param)
    return (z_out, grad_x, g_sc[0], g_wx, sums[S_BX], g_wy, sums[S_BY], sums[S_CW:S_CW + 4],
            sums[S_CB], g_wa[:chunks], sums[S_BA], g_wi, sums[S_BI], g_ap, g_wo, g_sc[1])


def solution(mesh):
    per_device = functools.partial(shard_body, cp_size=mesh.shape["cp"])
    return jax.shard_map(per_device, mesh=mesh, in_specs=IN_SPECS, out_specs=OUT_SPECS, check_vma=False)
```

```python
import functools
import jax
import jax.numpy as jnp
import numpy as np
from jax import lax
from jax.experimental import pallas as pl
from jax.experimental.pallas import tpu as pltpu
from jax.sharding import PartitionSpec as P

NORM_EPS = 1e-6
CONV_WIDTH = 4
BORROW = CONV_WIDTH - 1
LANES = 128
TB = 16
TINY = 1e-37
VMEM_BYTES = 66 * 1000 * 1000
F32 = jnp.float32
BF16 = jnp.bfloat16
IN_SPECS = (P(None, "cp", None), P(None, "cp", None), P(None, "cp"), P(), P(None, "tp"), P("tp"), P(None, "tp"), P("tp"), P(None, "tp"), P("tp"), P("tp", None, None), P("tp"), P("tp", None, None), P("tp"), P("tp"), P("tp", None), P())
OUT_SPECS = (P(None, "cp", None), P(None, "cp", None), P(), P(None, "tp"), P("tp"), P(None, "tp"), P("tp"), P(None, "tp"), P("tp"), P("tp", None, None), P("tp"), P("tp", None, None), P("tp"), P("tp"), P("tp", None), P())
V_BX, V_BY, V_CW, V_CB, V_BA, V_BI, V_SP = 0, 1, 2, 6, 7, 8, 9
S_BX, S_BY, S_CW, S_CB, S_BA, S_BI, S_AP = 0, 1, 2, 6, 7, 8, 9
LOG2E = 1.4426950408889634
RESET_LOG = -1e4
GELU_C = 0.7978845608028654
GELU_D = 0.044715


def dot_nn(lhs, rhs):
    return lax.dot_general(lhs, rhs, (((1,), (0,)), ((), ())), preferred_element_type=F32)


def dot_nt(lhs, rhs):
    return lax.dot_general(lhs, rhs, (((1,), (1,)), ((), ())), preferred_element_type=F32)


def dot_tn(lhs, rhs):
    return lax.dot_general(lhs, rhs, (((0,), (0,)), ((), ())), preferred_element_type=F32)


def sigm_scaled(val, bias):
    root = lax.rsqrt(1.0 + jnp.exp2(val * (-LOG2E) + bias))
    return root * root


def fold8(val):
    return (val[0:8] + val[8:16]) + (val[16:24] + val[24:32])


def to_time_major(perm, src_ref, dst_ref):
    n_seq, _, width = src_ref.shape
    for h in range(n_seq // TB):
        rows = src_ref[h * TB:(h + 1) * TB].reshape(TB * TB, width)
        dst_ref[:, h * TB:(h + 1) * TB, :] = dot_nn(perm, rows).astype(BF16).reshape(TB, TB, width)


def to_batch_major(perm, src_ref, dst_ref):
    n_seq, width = src_ref.shape[1], src_ref.shape[2]
    for h in range(n_seq // TB):
        rows = src_ref[:, h * TB:(h + 1) * TB, :].reshape(TB * TB, width)
        dst_ref[h * TB:(h + 1) * TB] = dot_nn(perm, rows).astype(BF16).reshape(TB, TB, width)


def norm_rows(xf, gain):
    rs = lax.rsqrt(jnp.mean(xf * xf, axis=-1, keepdims=True) + NORM_EPS)
    return (xf * rs * gain).astype(BF16)


def chunk_vec(vec_ref, col):
    return lambda row: vec_ref[row:row + 1, col]


def gate_terms(pa, pi, vec, cap):
    r = sigm_scaled(pa, vec(V_BA))
    i = sigm_scaled(pi, vec(V_BI))
    log_a = jnp.minimum(vec(V_SP) * r, cap)
    a = jnp.exp(log_a)
    a2 = a * a
    m2 = jnp.tanh(log_a) * (-1.0 - a2)
    inv_m = lax.rsqrt(jnp.maximum(m2, TINY))
    return r, i, log_a, a, a2, m2 * inv_m, inv_m


def gelu_parts(p):
    p2 = p * p
    half = 0.5 * jnp.tanh(p * (GELU_C + (GELU_C * GELU_D) * p2)) + 0.5
    y = p * half
    slope = half + y * (1.0 - half) * (2.0 * GELU_C + (6.0 * GELU_C * GELU_D) * p2)
    return y, slope


def gelu_only(p):
    return p * (0.5 * jnp.tanh(p * (GELU_C + (GELU_C * GELU_D) * (p * p))) + 0.5)


def fill_masks(pos_ref, mask_s):
    pos = pos_ref[...]
    mask_s[0] = jnp.where(pos == 0.0, RESET_LOG, 0.0)
    for k in range(1, CONV_WIDTH):
        mask_s[k] = jnp.where(pos >= float(k), 1.0, 0.0)


def lane_slice(start):
    return pl.ds(pl.multiple_of(start, LANES), LANES)


def row_slice(t, n_seq):
    return pl.ds(pl.multiple_of(t * n_seq, n_seq), n_seq)


def rows_at(t, n_seq):
    return slice(t * n_seq, (t + 1) * n_seq) if isinstance(t, int) else row_slice(t, n_seq)


def conv_lanes(mask_s, vec_ref, xb_ref, c_ref, n_seq, chunks):
    def conv_lane(l, c0):
        col = lane_slice(l * LANES)
        vec = chunk_vec(vec_ref, col)
        old = [xb_ref[l, rows_at(BORROW - k, n_seq), :].astype(F32) for k in range(1, CONV_WIDTH)]
        for t in range(TB):
            r = rows_at(t, n_seq)
            x = xb_ref[l, rows_at(t + BORROW, n_seq), :].astype(F32)
            acc = vec(V_CB) + x * vec(V_CW)
            for k in range(1, CONV_WIDTH):
                acc = acc + (old[k - 1] * mask_s[k, r, :]) * vec(V_CW + k)
            c_ref[l, r, :] = acc.astype(BF16)
            old = [x] + old[:-1]
        return c0

    lax.fori_loop(0, chunks, conv_lane, 0)


def gate_products(wai_ref, c_ref, pa_ref, pi_ref):
    for blk in range(wai_ref.shape[0]):
        pre = dot_nn(c_ref[blk], wai_ref[blk])
        pa_ref[blk] = pre[:, :LANES]
        pi_ref[blk] = pre[:, LANES:]


def put_chunks(ref, val, row0):
    for blk in range(ref.shape[0]):
        ref[blk, row0:row0 + val.shape[0], :] = val[:, rows_at(blk, LANES)].astype(ref.dtype)


def local_kernel(x_ref, gz_ref, pos_ref, xh_ref, vec_ref, sc_ref, wx_ref, wy_ref, wo_ref, wai_ref, perm_ref,
                 s_ref, r_ref, info_ref, xt_ref, gt_ref, n_ref, xb_ref, c_ref, py_ref, dm_ref, pa_ref, pi_ref,
                 nt_s, xbt_s, st_s, mask_s):
    n_seq, _, width = x_ref.shape
    own = wx_ref.shape[1]
    chunks = own // LANES
    rows = TB * n_seq
    halo = BORROW * n_seq
    perm = perm_ref[...]

    @pl.when(pl.program_id(0) == 0)
    def _():
        st_s[...] = jnp.zeros_like(st_s)
        st_s[1] = jnp.ones_like(st_s[1])
        for k in range(BORROW):
            nt_s[rows_at(k, n_seq), :] = norm_rows(xh_ref[rows_at(k, n_seq), :], sc_ref[:1, :])
        put_chunks(xbt_s, dot_nn(nt_s[...], wx_ref[...]) + vec_ref[V_BX:V_BX + 1, :], 0)

    to_time_major(perm, x_ref, xt_ref)
    to_time_major(perm, gz_ref, gt_ref)
    n_ref[0, :halo, :] = nt_s[...]
    xb_ref[0, :, :halo, :] = xbt_s[...]

    fill_masks(pos_ref, mask_s)
    part = 4

    def norm_part(q, c):
        for k in range(part):
            t = q * part + k
            n_ref[0, row_slice(t + BORROW, n_seq), :] = norm_rows(xt_ref[t].astype(F32), sc_ref[:1, :])
        return c

    lax.fori_loop(0, TB // part, norm_part, 0)
    n_blk = n_ref[0, halo:, :]
    put_chunks(xb_ref.at[0], dot_nn(n_blk, wx_ref[...]) + vec_ref[V_BX:V_BX + 1, :], halo)
    put_chunks(py_ref, dot_nn(n_blk, wy_ref[...]), 0)
    put_chunks(dm_ref, dot_nt(gt_ref[...].reshape(rows, width), wo_ref[...]), 0)
    nt_s[...] = n_ref[0, rows:, :]
    xbt_s[...] = xb_ref[0, :, rows:, :]
    conv_lanes(mask_s, vec_ref, xb_ref.at[0], c_ref, n_seq, chunks)
    gate_products(wai_ref, c_ref, pa_ref, pi_ref)

    def scan_lane(l, c0):
        col = lane_slice(l * LANES)
        vec = chunk_vec(vec_ref, col)

        h, p, hg = [st_s[k, :, col] for k in range(3)]
        for t in range(TB):
            r = rows_at(t, n_seq)
            _, i, _, a, _, m, _ = gate_terms(pa_ref[l, r, :], pi_ref[l, r, :], vec, mask_s[0, r, :])
            h = a * h + m * i * c_ref[l, r, :].astype(F32)
            p = a * p
            hg = hg + p * (dm_ref[l, r, :] * gelu_only(py_ref[l, r, :] + vec(V_BY)))
        for k, val in enumerate((h, p, hg)):
            st_s[k, :, col] = val
        return c0

    lax.fori_loop(0, chunks, scan_lane, 0)
    s_ref[0] = st_s[0]
    r_ref[0] = st_s[1]
    info_ref[...] = st_s[...]


def far_kernel(n_ref, gt_ref, pos_ref, vec_ref, wxy_ref, wo_ref, wai_ref, c_ref, py_ref, dm_ref, pa_ref, pi_ref, xb_s, mask_s):
    n_seq, width = gt_ref.shape[1], gt_ref.shape[2]
    own = wo_ref.shape[0]
    rows = TB * n_seq
    halo = BORROW * n_seq

    @pl.when(pl.program_id(0) == 0)
    def _():
        put_chunks(xb_s, dot_nn(n_ref[0, :halo, :], wxy_ref[:, :own]) + vec_ref[V_BX:V_BX + 1, :], rows)

    xb_s[:, :halo, :] = xb_s[:, rows:, :]
    fill_masks(pos_ref, mask_s)
    n_blk = n_ref[0, halo:, :]
    put_chunks(xb_s, dot_nn(n_blk, wxy_ref[:, :own]) + vec_ref[V_BX:V_BX + 1, :], halo)
    put_chunks(py_ref, dot_nn(n_blk, wxy_ref[:, own:]), 0)
    put_chunks(dm_ref, dot_nt(gt_ref[...].reshape(rows, width), wo_ref[...]), 0)
    conv_lanes(mask_s, vec_ref, xb_s, c_ref, n_seq, own // LANES)
    gate_products(wai_ref, c_ref, pa_ref, pi_ref)


def compose_kernel(info_ref, _, out_ref, *, cp_size):
    cp_index = lax.axis_index("cp")
    tp_index = lax.axis_index("tp")
    n_seq, own = info_ref.shape[2], info_ref.shape[3]
    for side in range(2):
        base = jnp.where(side == 0, tp_index, 1 - tp_index) * cp_size
        state = jnp.zeros((n_seq, own), F32)
        grad = jnp.zeros((n_seq, own), F32)
        for q in range(cp_size):
            state = jnp.where(q < cp_index, info_ref[base + q, 1] * state + info_ref[base + q, 0], state)
        for q in range(cp_size - 1, -1, -1):
            grad = jnp.where(q > cp_index, info_ref[base + q, 1] * grad + info_ref[base + q, 2], grad)
        out_ref[0, :, rows_at(side, own)] = state
        out_ref[1, :, rows_at(side, own)] = grad


def norm_back(xf, dn, gain):
    rs = lax.rsqrt(jnp.mean(xf * xf, axis=-1, keepdims=True) + NORM_EPS)
    xh = xf * rs
    dg = dn * xh
    dx = rs * (dn * gain - xh * jnp.mean(dg * gain, axis=-1, keepdims=True))
    return dx, fold8(dg)


def main_kernel(gt_ref, n_ref, xb_ref, pos_ref, c0_ref, c1_ref, py0_ref, py1_ref, dm0_ref, dm1_ref, pa0_ref, pa1_ref, pi0_ref, pi1_ref,
                s0_ref, r0_ref, s1_ref, r1_ref, st_ref, vec_ref, sc_ref, wxy_ref, wai_ref, xh_ref,
                mix_ref, d_ref, gwx_ref, gwy_ref, gwo_ref, gwa_ref, gwi_ref, dxh_ref, gsh_ref,
                dpai_s, g_s, a_s, ka_s, ki_s, k1_s, k3_s, e_s, dh_s, gvec_s, mask_s):
    n_seq, width = gt_ref.shape[1], gt_ref.shape[2]
    chunks = c0_ref.shape[0]
    own = chunks * LANES
    rows = TB * n_seq
    halo = BORROW * n_seq
    step = pl.program_id(0)
    last = step == pl.num_programs(0) - 1

    @pl.when(step == 0)
    def _():
        e_s[...] = jnp.zeros_like(e_s)
        dh_s[...] = st_ref[1]
        for ref in (gwx_ref, gwy_ref, gwo_ref, gwa_ref, gwi_ref, gvec_s):
            ref[...] = jnp.zeros_like(ref)

    fill_masks(pos_ref, mask_s)
    g_rows = gt_ref[...].reshape(rows, width)

    def fwd_lane(side):
        c_ref, py_ref, dm_ref, pa_ref, pi_ref, s_ref, r_ref = ((c0_ref, py0_ref, dm0_ref, pa0_ref, pi0_ref, s0_ref, r0_ref), (c1_ref, py1_ref, dm1_ref, pa1_ref, pi1_ref, s1_ref, r1_ref))[side]

        def run(l, c0):
            loc = lane_slice(l * LANES)
            col = lane_slice(l * LANES + side * own)
            cola = lane_slice(2 * (l * LANES + side * own))
            coli = lane_slice(2 * (l * LANES + side * own) + LANES)
            coly = lane_slice(l * LANES + (2 * side + 1) * own)
            vec = chunk_vec(vec_ref, col)
            state = st_ref[0, :, col]
            state = jnp.where(last, state, s_ref[0, :, loc] + r_ref[0, :, loc] * state)

            h, s_by = state, jnp.zeros((8, LANES), F32)
            for t in range(TB):
                r = rows_at(t, n_seq)
                rg, i, log_a, a, a2, m, inv_m = gate_terms(pa_ref[l, r, :], pi_ref[l, r, :], vec, mask_s[0, r, :])
                cf = c_ref[l, r, :].astype(F32)
                k1 = m * i
                u = k1 * cf
                ah = a * h
                k3r = (ah - (i * cf) * (a2 * inv_m)) * rg
                h = ah + u
                y, slope = gelu_parts(py_ref[l, r, :] + vec(V_BY))
                dm = dm_ref[l, r, :]
                mix_ref[r, col] = (h * y).astype(BF16)
                dpy = dm * h * slope
                d_ref[r, coly] = dpy.astype(BF16)
                g_s[l + side * chunks, r, :] = dm * y
                a_s[l + side * chunks, r, :] = a
                k1_s[l + side * chunks, r, :] = k1
                ka_s[l + side * chunks, r, :] = k3r * (vec(V_SP) - log_a)
                ki_s[l + side * chunks, r, :] = u * (1.0 - i)
                if side == 0:
                    k3_s[l + side * chunks, r, :] = k3r
                    s_by = s_by + fold8(dpy)
            if side == 0:
                gvec_s[S_BY, :, col] += s_by
            return c0

        return run

    lax.fori_loop(0, chunks, fwd_lane(0), 0)
    lax.fori_loop(0, chunks, fwd_lane(1), 0)
    gwo_ref[...] += dot_tn(mix_ref[:, :own], g_rows)

    def bwd_lane(side):
        def run(l, c0):
            col = lane_slice(l * LANES + side * own)
            cola = lane_slice(2 * (l * LANES + side * own))
            coli = lane_slice(2 * (l * LANES + side * own) + LANES)

            def body(tt, carry):
                nxt, s_a, s_i, s_p = carry
                r = row_slice(TB - 1 - tt, n_seq)
                dh = g_s[l + side * chunks, r, :] + nxt
                nxt = a_s[l + side * chunks, r, :] * dh
                dpa = dh * ka_s[l + side * chunks, r, :]
                dpi = dh * ki_s[l + side * chunks, r, :]
                g_s[l + side * chunks, r, :] = dh * k1_s[l + side * chunks, r, :]
                dpai_s[l + side * chunks, r, :LANES] = dpa.astype(BF16)
                dpai_s[l + side * chunks, r, LANES:] = dpi.astype(BF16)
                if side == 0:
                    s_a = s_a + fold8(dpa)
                    s_i = s_i + fold8(dpi)
                    s_p = s_p + fold8(dh * k3_s[l + side * chunks, r, :])
                return nxt, s_a, s_i, s_p

            zero = jnp.zeros((8, LANES), F32)
            nxt, s_a, s_i, s_p = lax.fori_loop(0, TB, body, (dh_s[:, col], zero, zero, zero), unroll=8)
            dh_s[:, col] = nxt
            if side == 0:
                gvec_s[S_BA, :, col] += s_a
                gvec_s[S_BI, :, col] += s_i
                gvec_s[S_AP, :, col] += s_p
            return c0

        return run

    lax.fori_loop(0, chunks, bwd_lane(0), 0)
    lax.fori_loop(0, chunks, bwd_lane(1), 0)

    for blk in range(2 * chunks):
        g_s[blk] += dot_nt(dpai_s[blk], wai_ref[blk])
        if blk < chunks:
            g_ai = dot_tn(c0_ref[blk], dpai_s[blk])
            gwa_ref[blk] += g_ai[:, :LANES]
            gwi_ref[blk] += g_ai[:, LANES:]

    def convb_lane(side):
        def run(l, c0):
            col = lane_slice(l * LANES + side * own)
            colx = lane_slice(l * LANES + 2 * side * own)
            vec = chunk_vec(vec_ref, col)

            e3, e2, e1 = [e_s[rows_at(k, n_seq), col] for k in range(BORROW)]
            s_b = s_x = jnp.zeros((8, LANES), F32)
            taps = [s_b] * CONV_WIDTH
            if side == 0:
                xs = [xb_ref[0, l, rows_at(TB - 1 + BORROW - k, n_seq), :].astype(F32) for k in range(BORROW)]
            dc_next = g_s[l + side * chunks, rows_at(TB - 1, n_seq), :]
            for t in range(TB - 1, -1, -1):
                r = rows_at(t, n_seq)
                dc, dc_next = dc_next, g_s[l + side * chunks, rows_at(max(t - 1, 0), n_seq), :]
                dm = [dc] + [dc * mask_s[k, r, :] for k in range(1, CONV_WIDTH)]
                dx = e1 + dc * vec(V_CW)
                e1 = e2 + dm[1] * vec(V_CW + 1)
                e2 = e3 + dm[2] * vec(V_CW + 2)
                e3 = dm[3] * vec(V_CW + 3)
                d_ref[r, colx] = dx.astype(BF16)
                if side == 0:
                    s_b = s_b + fold8(dc)
                    s_x = s_x + fold8(dx)
                    xs = xs + [xb_ref[0, l, rows_at(t, n_seq), :].astype(F32)]
                    taps = [acc + fold8(dm[k] * xs[k]) for k, acc in enumerate(taps)]
                    xs = xs[1:]
            for k, val in enumerate((e3, e2, e1)):
                e_s[rows_at(k, n_seq), col] = val
            if side == 0:
                gvec_s[S_CB, :, col] += s_b
                gvec_s[S_BX, :, col] += s_x
                for k in range(CONV_WIDTH):
                    gvec_s[S_CW + k, :, col] += taps[k]
            return c0

        return run

    lax.fori_loop(0, chunks, convb_lane(0), 0)
    lax.fori_loop(0, chunks, convb_lane(1), 0)
    n_blk = n_ref[0, halo:, :]
    g_both = dot_tn(n_blk, d_ref[:, :2 * own])
    gwx_ref[...] += g_both[:, :own]
    gwy_ref[...] += g_both[:, own:]

    @pl.when(last)
    def _():
        e16 = e_s[...].astype(BF16)
        gwx_ref[...] += dot_tn(n_ref[0, :halo, :], e16[:, :own])
        for k in range(BORROW):
            gvec_s[S_BX] += fold8(e_s[rows_at(k, n_seq), :own])
        dn = dot_nt(e16[:, :own], wxy_ref[:, :own]) + dot_nt(e16[:, own:], wxy_ref[:, 2 * own:3 * own])
        s_g = jnp.zeros((8, width), F32)
        for k in range(BORROW):
            sl = rows_at(k, n_seq)
            dx, sg = norm_back(xh_ref[sl, :], dn[sl], sc_ref[:1, :])
            s_g = s_g + sg
            dxh_ref[sl, :] = dx
        gsh_ref[...] = s_g
        sums = jnp.sum(gvec_s[...], axis=1)
        for q in range(chunks):
            gwa_ref[chunks, q * 16:q * 16 + sums.shape[0], :] = sums[:, q * LANES:(q + 1) * LANES]


def out_kernel(mix_ref, d_ref, xt_ref, gt_ref, fix_ref, gsh_ref, sc_ref, wxy_ref, wo_ref, perm_ref, z_ref, gx_ref, gsc_ref, o_s, q_s, zt_s, gxt_s):
    n_seq, width = xt_ref.shape[1], xt_ref.shape[2]
    rows = TB * n_seq
    halo = BORROW * n_seq
    perm = perm_ref[...]
    step = pl.program_id(0)

    @pl.when(step == 0)
    def _():
        gsc_ref[0] = gsh_ref[...]
        gsc_ref[1] = jnp.zeros((8, width), F32)

    q_s[...] = dot_nt(d_ref[...], wxy_ref[...])
    part = 4

    def gx_part(q, c):
        rp = pl.ds(pl.multiple_of(q * part * n_seq, part * n_seq), part * n_seq)
        o_s[rp, :] = dot_nn(mix_ref[rp, :], wo_ref[...])
        for k in range(part):
            t = q * part + k
            r = row_slice(t, n_seq)
            dx, sg = norm_back(xt_ref[t].astype(F32), q_s[r, :], sc_ref[:1, :])
            gzf = gt_ref[t].astype(F32)
            gx = gzf + dx
            q_s[r, :] = gx
            gxt_s[t] = gx.astype(BF16)
            gsc_ref[0] += sg
            gsc_ref[1] += fold8(gzf)
        return c

    lax.fori_loop(0, TB // part, gx_part, 0)

    @pl.when(step == pl.num_programs(0) - 1)
    def _():
        tail = q_s[rows - halo:, :] + fix_ref[...]
        gxt_s[TB - BORROW:] = tail.astype(BF16).reshape(BORROW, n_seq, width)

    def z_rows(t, c):
        zt_s[t] = (xt_ref[t].astype(F32) + (o_s[row_slice(t, n_seq), :] + sc_ref[1:2, :])).astype(BF16)
        return c

    lax.fori_loop(0, TB, z_rows, 0, unroll=2)
    to_batch_major(perm, zt_s, z_ref)
    to_batch_major(perm, gxt_s, gx_ref)


def pack_kernel(wx_ref, wy_ref, wo_ref, wa_ref, wi_ref, bx_ref, by_ref, cw_ref, cb_ref, ba_ref, bi_ref, sp_ref, half_ref, vec_ref, wai_ref):
    width, own = wx_ref.shape
    n_blk = wa_ref.shape[0]
    wai_ref[:, :, :LANES] = wa_ref[...]
    wai_ref[:, :, LANES:] = wi_ref[...]
    vec_ref[V_BX:V_BX + 1, :] = bx_ref[...].astype(F32).reshape(1, own)
    vec_ref[V_BY:V_BY + 1, :] = by_ref[...].astype(F32).reshape(1, own)
    vec_ref[V_CW:V_CW + CONV_WIDTH, :] = cw_ref[...].astype(F32)
    vec_ref[V_CB:V_CB + 1, :] = cb_ref[...].astype(F32).reshape(1, own)
    vec_ref[V_BA:V_BA + 1, :] = ba_ref[...].astype(F32).reshape(1, own) * (-LOG2E)
    vec_ref[V_BI:V_BI + 1, :] = bi_ref[...].astype(F32).reshape(1, own) * (-LOG2E)
    vec_ref[V_SP:V_SP + 1, :] = sp_ref[...].reshape(1, own)
    vec_ref[V_SP + 1:, :] = jnp.zeros((15 - V_SP, own), F32)
    for side, w_ref in enumerate((wx_ref, wy_ref)):
        @pl.when(lax.rem(lax.axis_index("cp"), 2) == side)
        def _():
            half_ref[:width, :] = w_ref[...].astype(F32)
            half_ref[width:width + own, :] = wo_ref[:, rows_at(side, own)].astype(F32)
            for k in range(n_blk // 2):
                blk = side * (n_blk // 2) + k
                half_ref[width + own:width + own + LANES, rows_at(2 * k, LANES)] = wa_ref[blk].astype(F32)
                half_ref[width + own:width + own + LANES, rows_at(2 * k + 1, LANES)] = wi_ref[blk].astype(F32)
            half_ref[width + own + LANES:, :] = vec_ref[rows_at(side, 8), :]


def assemble_kernel(wx_ref, wy_ref, wo_ref, wai_ref, vec_ref, mine_ref, other_ref, wxy_out, wo_out, wai_out, vec_out):
    width, own = wx_ref.shape
    n_blk = wai_ref.shape[0]
    wxy_out[:, :own] = wx_ref[...]
    wxy_out[:, own:2 * own] = wy_ref[...]
    wo_out[:own, :] = wo_ref[...]
    wai_out[:n_blk] = wai_ref[...]
    vec_out[:, :own] = vec_ref[...]
    parity = lax.rem(lax.axis_index("cp"), 2)
    for side in range(2):
        for ref, want in ((mine_ref, side), (other_ref, 1 - side)):
            @pl.when(parity == want)
            def _():
                wxy_out[:, (2 + side) * own:(3 + side) * own] = ref[:width, :].astype(BF16)
                wo_out[own:, rows_at(side, own)] = ref[width:width + own, :].astype(BF16)
                for k in range(n_blk // 2):
                    wai_out[n_blk + side * (n_blk // 2) + k] = ref[width + own:width + own + LANES, 2 * k * LANES:(2 * k + 2) * LANES].astype(BF16)
                vec_out[rows_at(side, 8), own:] = ref[width + own + LANES:, :]


def unpack_kernel(wx_ref, wy_ref, wo_ref, wa_ref, wi_ref, wx_out, wy_out, wo_out, wa_out, wi_out, sum_out):
    chunks = wi_ref.shape[0]
    wx_out[...] = wx_ref[...]
    wy_out[...] = wy_ref[...]
    wo_out[...] = wo_ref[...]
    wa_out[...] = wa_ref[:chunks]
    wi_out[...] = wi_ref[...]
    for q in range(chunks):
        sum_out[:, rows_at(q, LANES)] = wa_ref[chunks, rows_at(q, 16), :]


def const_spec(shape):
    return pl.BlockSpec(shape, lambda j: (0,) * len(shape), pipeline_mode=pl.Buffered(1))


def shard_body(x_in, grad_z, seg_pos, norm_scale, w_x, b_x, w_y, b_y, conv_w, conv_b, w_a, b_a, w_i, b_i, a_param, w_out, b_out, cp_size):
    n_seq, n_tok, width = x_in.shape
    own = w_x.shape[1]
    full = 2 * own
    nb = n_tok // TB
    rows = TB * n_seq
    halo = BORROW * n_seq
    chunks = own // LANES
    fwd_perm = list(zip(range(cp_size - 1), range(1, cp_size)))
    back_perm = [(b, a) for a, b in fwd_perm]
    swap = [(0, 1), (1, 0)]

    x_tail = x_in[:, n_tok - BORROW:, :].astype(F32).transpose(1, 0, 2).reshape(halo, width)
    x_halo = lax.ppermute(x_tail, "cp", fwd_perm)

    sp8 = -8.0 * jax.nn.softplus(a_param)
    half, vec_own, w_ai = pl.pallas_call(
        pack_kernel,
        out_shape=[jax.ShapeDtypeStruct((width + own + LANES + 8, own), F32), jax.ShapeDtypeStruct((16, own), F32), jax.ShapeDtypeStruct((chunks, LANES, 2 * LANES), BF16)],
        compiler_params=pltpu.CompilerParams(vmem_limit_bytes=VMEM_BYTES),
        name="pack",
    )(w_x, w_y, w_out, w_a, w_i, b_x, b_y, conv_w, conv_b, b_a, b_i, sp8)
    far_half = lax.ppermute(half, "tp", swap)
    far_other = lax.ppermute(far_half, "cp", [(d, d ^ 1) for d in range(cp_size)])

    pos = jnp.broadcast_to(seg_pos.T.astype(F32).reshape(n_tok * n_seq, 1), (n_tok * n_seq, LANES))
    scales = jnp.concatenate([1.0 + norm_scale.astype(F32)[None], b_out.astype(F32)[None], jnp.zeros((6, width), F32)], axis=0)
    line = np.arange(TB * TB)
    perm = jnp.asarray((line[:, None] // TB == line[None, :] % TB) & (line[:, None] % TB == line[None, :] // TB), BF16)

    def vmem(shape, dtype):
        return pltpu.VMEM(shape, dtype)

    def sds(shape, dtype):
        return jax.ShapeDtypeStruct(shape, dtype)

    params = pltpu.CompilerParams(vmem_limit_bytes=VMEM_BYTES, dimension_semantics=("arbitrary",))

    def cost(gflop):
        return pl.CostEstimate(flops=gflop * 10 ** 9, bytes_accessed=10 ** 8, transcendentals=0)

    def blocks(idx):
        batch = pl.BlockSpec((n_seq, TB, width), lambda j: (0, idx(j), 0))
        time = pl.BlockSpec((TB, n_seq, width), lambda j: (idx(j), 0, 0))
        row = lambda cols: pl.BlockSpec((rows, cols), lambda j: (idx(j), 0))
        per = lambda *dims: pl.BlockSpec((1,) + dims, lambda j: (idx(j), 0, 0))
        chk = pl.BlockSpec((chunks, rows, LANES), lambda j: (0, idx(j), 0))
        xbs = pl.BlockSpec((1, chunks, rows + halo, LANES), lambda j: (idx(j), 0, 0, 0))
        return batch, time, row, per, chk, xbs

    batch, time, row, per, chk, xbs = blocks(lambda j: j)
    tok = n_tok * n_seq
    ends, prods, info, xt, gt, n_all, xb, c_own, py_own, dm_own, pa_own, pi_own = pl.pallas_call(
        local_kernel,
        grid=(nb,),
        in_specs=[batch, batch, row(LANES), const_spec((halo, width)), const_spec((16, own)), const_spec((8, width)),
                  const_spec((width, own)), const_spec((width, own)), const_spec((own, width)), const_spec(w_ai.shape), const_spec(perm.shape)],
        out_specs=[per(n_seq, own), per(n_seq, own), const_spec((3, n_seq, own)), time, time, per(rows + halo, width), xbs,
                   chk, chk, chk, chk, chk],
        out_shape=[sds((nb, n_seq, own), F32), sds((nb, n_seq, own), F32), sds((3, n_seq, own), F32), sds((n_tok, n_seq, width), BF16), sds((n_tok, n_seq, width), BF16),
                   sds((nb, rows + halo, width), BF16), sds((nb, chunks, rows + halo, LANES), BF16), sds((chunks, tok, LANES), BF16)] + [sds((chunks, tok, LANES), F32)] * 4,
        scratch_shapes=[vmem((halo, width), BF16), vmem((chunks, halo, LANES), BF16), vmem((3, n_seq, own), F32), vmem((CONV_WIDTH, rows, LANES), F32)],
        compiler_params=params, cost_estimate=cost(100), name="local_pass",
    )(x_in, grad_z, pos, x_halo, vec_own, scales, w_x, w_y, w_out, w_ai, perm)

    infos = lax.all_gather(info, ("tp", "cp"))
    far_ends = lax.ppermute(ends, "tp", swap)
    far_prods = lax.ppermute(prods, "tp", swap)

    w_xy, w_o, w_g, vec = pl.pallas_call(
        assemble_kernel,
        out_shape=[sds((width, 4 * own), BF16), sds((full, width), BF16), sds((2 * chunks,) + w_ai.shape[1:], BF16), sds((16, full), F32)],
        compiler_params=pltpu.CompilerParams(vmem_limit_bytes=VMEM_BYTES),
        name="assemble",
    )(w_x, w_y, w_out, w_ai, vec_own, far_half, far_other)

    c_far, py_far, dm_far, pa_far, pi_far = pl.pallas_call(
        far_kernel,
        grid=(nb,),
        in_specs=[per(rows + halo, width), time, row(LANES), pl.BlockSpec((16, own), lambda j: (0, 1), pipeline_mode=pl.Buffered(1)),
                  pl.BlockSpec((width, full), lambda j: (0, 1), pipeline_mode=pl.Buffered(1)), pl.BlockSpec((own, width), lambda j: (1, 0), pipeline_mode=pl.Buffered(1)),
                  pl.BlockSpec(w_ai.shape, lambda j: (1, 0, 0), pipeline_mode=pl.Buffered(1))],
        out_specs=[chk] * 5,
        out_shape=[sds((chunks, tok, LANES), BF16)] + [sds((chunks, tok, LANES), F32)] * 4,
        scratch_shapes=[vmem((chunks, rows + halo, LANES), BF16), vmem((CONV_WIDTH, rows, LANES), F32)],
        compiler_params=params, cost_estimate=cost(50), name="far_pass",
    )(n_all, gt, pos, vec, w_xy, w_o, w_g)

    states = pl.pallas_call(
        functools.partial(compose_kernel, cp_size=cp_size),
        in_specs=[pl.BlockSpec(memory_space=pltpu.VMEM), pl.BlockSpec(memory_space=pl.ANY)],
        out_shape=sds((2, n_seq, full), F32),
        compiler_params=pltpu.CompilerParams(vmem_limit_bytes=VMEM_BYTES),
        name="compose",
    )(infos, c_far)

    batch, time, row, per, chk, xbs = blocks(lambda j: nb - 1 - j)
    bound = pl.BlockSpec((1, n_seq, own), lambda j: (jnp.maximum(nb - 2 - j, 0), 0, 0))
    mix, d_all, g_wx, g_wy, g_wo, g_wa, g_wi, dx_halo, g_sh = pl.pallas_call(
        main_kernel,
        grid=(nb,),
        in_specs=[time, per(rows + halo, width), xbs, row(LANES)] + [chk] * 10 + [
                  bound, bound, bound, bound, const_spec((2, n_seq, full)), const_spec((16, full)), const_spec((8, width)),
                  const_spec((width, 2 * full)), const_spec(w_g.shape), const_spec((halo, width))],
        out_specs=[row(full), row(2 * full), const_spec((width, own)), const_spec((width, own)), const_spec((own, width)),
                   const_spec((chunks + 1, LANES, LANES)), const_spec((chunks, LANES, LANES)), const_spec((halo, width)), const_spec((8, width))],
        out_shape=[sds((tok, full), BF16), sds((tok, 2 * full), BF16), sds((width, own), F32), sds((width, own), F32), sds((own, width), F32),
                   sds((chunks + 1, LANES, LANES), F32), sds((chunks, LANES, LANES), F32), sds((halo, width), F32), sds((8, width), F32)],
        scratch_shapes=[vmem((2 * chunks, rows, 2 * LANES), BF16)] + [vmem((2 * chunks, rows, LANES), F32)] * 5 + [vmem((chunks, rows, LANES), F32), vmem((halo, full), F32), vmem((n_seq, full), F32), vmem((10, 8, own), F32), vmem((CONV_WIDTH, rows, LANES), F32)],
        compiler_params=params, cost_estimate=cost(300), name="main_pass",
    )(gt, n_all, xb, pos, c_own, c_far, py_own, py_far, dm_own, dm_far, pa_own, pa_far, pi_own, pi_far, ends, prods, far_ends, far_prods, states, vec, scales, w_xy, w_g, x_halo)

    fix = lax.ppermute(dx_halo, "cp", back_perm)
    g_wx, g_wy, g_wo, g_wa, g_wi = lax.psum((g_wx, g_wy, g_wo, g_wa, g_wi), "cp")

    batch, time, row, per, chk, xbs = blocks(lambda j: j)
    z_out, grad_x, g_sc = pl.pallas_call(
        out_kernel,
        grid=(nb,),
        in_specs=[row(full), row(2 * full), time, time, const_spec((halo, width)), const_spec((8, width)), const_spec((8, width)),
                  const_spec((width, 2 * full)), const_spec((full, width)), const_spec(perm.shape)],
        out_specs=[batch, batch, const_spec((2, 8, width))],
        out_shape=[sds(x_in.shape, BF16), sds(x_in.shape, BF16), sds((2, 8, width), F32)],
        scratch_shapes=[vmem((rows, width), F32), vmem((rows, width), F32), vmem((TB, n_seq, width), BF16), vmem((TB, n_seq, width), BF16)],
        compiler_params=params, cost_estimate=cost(100), name="out_pass",
    )(mix, d_all, xt, gt, fix, g_sh, scales, w_xy, w_o, perm)

    g_wx, g_wy, g_wo, g_wa, g_wi, sums = pl.pallas_call(
        unpack_kernel,
        out_shape=[sds(v.shape, F32) for v in (g_wx, g_wy, g_wo, g_wi, g_wi)] + [sds((16, own), F32)],
        compiler_params=pltpu.CompilerParams(vmem_limit_bytes=VMEM_BYTES), cost_estimate=cost(2), name="unpack",
    )(g_wx, g_wy, g_wo, g_wa, g_wi)

    g_sc = jnp.sum(g_sc, axis=1)
    hop = 1
    while hop < cp_size:
        g_sc = g_sc + lax.ppermute(g_sc, "cp", [(d, d ^ hop) for d in range(cp_size)])
        hop *= 2

    g_ap = sums[S_AP] * (-8.0) * jax.nn.sigmoid(a_param)
    return (z_out, grad_x, g_sc[0], g_wx, sums[S_BX], g_wy, sums[S_BY], sums[S_CW:S_CW + 4],
            sums[S_CB], g_wa, sums[S_BA], g_wi, sums[S_BI], g_ap, g_wo, g_sc[1])


def solution(mesh):
    per_device = functools.partial(shard_body, cp_size=mesh.shape["cp"])
    return jax.shard_map(per_device, mesh=mesh, in_specs=IN_SPECS, out_specs=OUT_SPECS, check_vma=False)
```
